8 devices in a mesh: rep: 1 (over z), mp: 2 (over y), tok: 4 (over x, core).
Axes of the slice: x: 2, y: 2, z: 1, core: 2. Of those that a mesh axis runs over, the one named last changes fastest.
Arguments:
- hidden_in: bfloat16 [16384, 768], P(('rep', 'tok', 'mp'))
- seg_ids: int32 [16384], P(('rep', 'tok', 'mp'))
- expert_ids: int32 [16384, 2], P(('rep', 'tok', 'mp'))
- expert_gates: float32 [16384, 2], P(('rep', 'tok', 'mp'))
- w_query: bfloat16 [2, 768, 12, 64], P(None, 'tok', 'mp')
- w_key: bfloat16 [2, 768, 12, 64], P(None, 'tok', 'mp')
- w_value: bfloat16 [2, 768, 12, 64], P(None, 'tok', 'mp')
- w_out: bfloat16 [2, 12, 64, 768], P(None, 'mp', None, 'tok')
- w_gate: bfloat16 [2, 8, 768, 3072], P(None, None, 'tok', 'mp')
- w_up: bfloat16 [2, 8, 768, 3072], P(None, None, 'tok', 'mp')
- w_down: bfloat16 [2, 8, 3072, 768], P(None, None, 'mp', 'tok')
- gain_attn: bfloat16 [2, 768], replicated
- gain_mlp: bfloat16 [2, 768], replicated
Outputs:
- output: float32 [16384, 768], P(('rep', 'tok', 'mp'))
All inputs are finite; a program needn't handle non-finite values.
Results may differ from the reference program's by a relative error of at most 0.0101443.
Values are sent between devices in bfloat16 or wider.
A program may use at most 1 GiB of HBM per device.

```python
import jax
import jax.numpy as jnp
from jax import lax

TOKENS = 16384
SHARDS = 4
HIDDEN = 768
FFN_WIDTH = 3072
Q_HEADS = 12
KV_HEADS = 12
HEAD_DIM = 64
EXPERTS = 8
NUM_LAYERS = 2
REQ_CUTS = 3

SHARD_LEN = TOKENS // SHARDS
QUERY_BLOCK = min(SHARD_LEN, 256)
EPS = 1e-5
ROPE_BASE = 10000.0


def normal_weight(key, shape, scale):
    return (jax.random.normal(key, shape, jnp.float32) * scale).astype(jnp.bfloat16)


def setup_inputs(seed: int = 0, part: int = 0) -> dict:
    base_key = jax.random.key(seed)
    part_keys = jax.random.split(jax.random.fold_in(base_key, part), 5)
    weight_keys = jax.random.split(jax.random.key(seed + 1), 9)
    hidden_in = jax.random.normal(part_keys[0], (TOKENS, HIDDEN), jnp.float32).astype(jnp.bfloat16)
    cut_points = jax.random.randint(part_keys[1], (SHARDS, 1, REQ_CUTS), 1, SHARD_LEN)
    token_pos = jnp.arange(SHARD_LEN, dtype=jnp.int32)[None, :, None]
    req_index = jnp.sum((token_pos >= cut_points).astype(jnp.int32), axis=-1)
    shard_base = jnp.arange(SHARDS, dtype=jnp.int32)[:, None] * (REQ_CUTS + 1)
    seg_ids = (shard_base + req_index).reshape(TOKENS).astype(jnp.int32)
    first_pick = jax.random.permutation(part_keys[2], jnp.arange(TOKENS, dtype=jnp.int32) % EXPERTS)
    pick_shift = jax.random.randint(part_keys[3], (TOKENS,), 1, EXPERTS)
    second_pick = (first_pick + pick_shift) % EXPERTS
    expert_ids = jnp.stack([first_pick, second_pick], axis=1).astype(jnp.int32)
    top_share = jax.random.uniform(part_keys[4], (TOKENS,), jnp.float32, 0.3, 0.9)
    expert_gates = jnp.stack([top_share, 1.0 - top_share], axis=1)
    qk_scale = 1.4 * HIDDEN ** -0.5
    return {
        'hidden_in': hidden_in,
        'seg_ids': seg_ids,
        'expert_ids': expert_ids,
        'expert_gates': expert_gates,
        'w_query': normal_weight(weight_keys[0], (NUM_LAYERS, HIDDEN, Q_HEADS, HEAD_DIM), qk_scale),
        'w_key': normal_weight(weight_keys[1], (NUM_LAYERS, HIDDEN, KV_HEADS, HEAD_DIM), qk_scale),
        'w_value': normal_weight(weight_keys[2], (NUM_LAYERS, HIDDEN, KV_HEADS, HEAD_DIM), HIDDEN ** -0.5),
        'w_out': normal_weight(weight_keys[3], (NUM_LAYERS, Q_HEADS, HEAD_DIM, HIDDEN), 2.0 * (Q_HEADS * HEAD_DIM) ** -0.5),
        'w_gate': normal_weight(weight_keys[4], (NUM_LAYERS, EXPERTS, HIDDEN, FFN_WIDTH), HIDDEN ** -0.5),
        'w_up': normal_weight(weight_keys[5], (NUM_LAYERS, EXPERTS, HIDDEN, FFN_WIDTH), HIDDEN ** -0.5),
        'w_down': normal_weight(weight_keys[6], (NUM_LAYERS, EXPERTS, FFN_WIDTH, HIDDEN), FFN_WIDTH ** -0.5),
        'gain_attn': jax.random.uniform(weight_keys[7], (NUM_LAYERS, HIDDEN), jnp.float32, 0.5, 1.5).astype(jnp.bfloat16),
        'gain_mlp': jax.random.uniform(weight_keys[8], (NUM_LAYERS, HIDDEN), jnp.float32, 0.5, 1.5).astype(jnp.bfloat16),
    }


def rms_norm(residual, gain):
    inv_rms = lax.rsqrt(jnp.mean(residual * residual, axis=-1, keepdims=True) + EPS)
    return (residual * inv_rms * gain.astype(jnp.float32)).astype(jnp.bfloat16)


def request_positions(seg_shard):
    token_index = jnp.arange(SHARD_LEN, dtype=jnp.int32)
    is_start = jnp.concatenate([jnp.ones((1,), dtype=jnp.bool_), seg_shard[1:] != seg_shard[:-1]])
    start_index = lax.cummax(jnp.where(is_start, token_index, 0), axis=0)
    return token_index - start_index


def apply_rope(vectors, positions):
    half_dim = HEAD_DIM // 2
    inv_freq = jnp.power(ROPE_BASE, -jnp.arange(half_dim, dtype=jnp.float32) * 2.0 / HEAD_DIM)
    angles = positions.astype(jnp.float32)[:, None, None] * inv_freq
    cosines = jnp.cos(angles)
    sines = jnp.sin(angles)
    first_half = vectors[..., :half_dim]
    second_half = vectors[..., half_dim:]
    return jnp.concatenate([first_half * cosines - second_half * sines, second_half * cosines + first_half * sines], axis=-1)


def shard_attention(h_shard, seg_shard, q_weight, k_weight, v_weight):
    groups = Q_HEADS // KV_HEADS
    positions = request_positions(seg_shard)
    q_proj = jnp.dot(h_shard, q_weight.reshape(HIDDEN, Q_HEADS * HEAD_DIM), preferred_element_type=jnp.float32)
    k_proj = jnp.dot(h_shard, k_weight.reshape(HIDDEN, KV_HEADS * HEAD_DIM), preferred_element_type=jnp.float32)
    v_proj = jnp.dot(h_shard, v_weight.reshape(HIDDEN, KV_HEADS * HEAD_DIM), preferred_element_type=jnp.float32)
    q_rot = apply_rope(q_proj.reshape(SHARD_LEN, Q_HEADS, HEAD_DIM), positions).astype(jnp.bfloat16)
    k_rot = apply_rope(k_proj.reshape(SHARD_LEN, KV_HEADS, HEAD_DIM), positions).astype(jnp.bfloat16)
    keys32 = k_rot.astype(jnp.float32)
    values32 = v_proj.astype(jnp.bfloat16).astype(jnp.float32).reshape(SHARD_LEN, KV_HEADS, HEAD_DIM)
    token_index = jnp.arange(SHARD_LEN, dtype=jnp.int32)
    num_blocks = SHARD_LEN // QUERY_BLOCK
    q_blocks = q_rot.reshape(num_blocks, QUERY_BLOCK, KV_HEADS, groups, HEAD_DIM)

    def one_block(block_in):
        q_block, seg_block, index_block = block_in
        scores = jnp.einsum('bhgd,shd->hgbs', q_block.astype(jnp.float32), keys32) * HEAD_DIM ** -0.5
        allowed = (seg_block[:, None] == seg_shard[None, :]) & (token_index[None, :] <= index_block[:, None])
        attn_prob = jax.nn.softmax(jnp.where(allowed, scores, -1e30), axis=-1)
        attn_prob = attn_prob.astype(jnp.bfloat16).astype(jnp.float32)
        attn_out = jnp.einsum('hgbs,shd->bhgd', attn_prob, values32)
        return attn_out.astype(jnp.bfloat16).reshape(QUERY_BLOCK, Q_HEADS * HEAD_DIM)

    block_outs = lax.map(one_block, (q_blocks, seg_shard.reshape(num_blocks, QUERY_BLOCK), token_index.reshape(num_blocks, QUERY_BLOCK)))
    return block_outs.reshape(SHARD_LEN, Q_HEADS * HEAD_DIM)


def expert_mix(normed, expert_ids, expert_gates, gate_weight, up_weight, down_weight):
    def one_expert(mix_sum, expert_in):
        gate_mat, up_mat, down_mat, expert_num = expert_in
        gate_pre = jnp.dot(normed, gate_mat, preferred_element_type=jnp.float32)
        up_pre = jnp.dot(normed, up_mat, preferred_element_type=jnp.float32)
        hidden_act = (jax.nn.silu(gate_pre) * up_pre).astype(jnp.bfloat16)
        down_out = jnp.dot(hidden_act, down_mat, preferred_element_type=jnp.float32)
        route_weight = jnp.sum(jnp.where(expert_ids == expert_num, expert_gates, 0.0), axis=1)
        return mix_sum + route_weight[:, None] * down_out, None

    start_sum = jnp.zeros((normed.shape[0], HIDDEN), jnp.float32)
    mix_sum, _ = lax.scan(one_expert, start_sum, (gate_weight, up_weight, down_weight, jnp.arange(EXPERTS, dtype=jnp.int32)))
    return mix_sum


def reference(hidden_in, seg_ids, expert_ids, expert_gates, w_query, w_key, w_value, w_out, w_gate, w_up, w_down, gain_attn, gain_mlp):
    seg_shards = seg_ids.reshape(SHARDS, SHARD_LEN)

    def one_layer(residual, layer_in):
        q_weight, k_weight, v_weight, o_weight, gate_weight, up_weight, down_weight, attn_gain, mlp_gain = layer_in
        normed = rms_norm(residual, attn_gain).reshape(SHARDS, SHARD_LEN, HIDDEN)
        attn_out = lax.map(lambda shard_in: shard_attention(shard_in[0], shard_in[1], q_weight, k_weight, v_weight), (normed, seg_shards))
        attn_out = attn_out.reshape(TOKENS, Q_HEADS * HEAD_DIM)
        residual = residual + jnp.dot(attn_out, o_weight.reshape(Q_HEADS * HEAD_DIM, HIDDEN), preferred_element_type=jnp.float32)
        normed = rms_norm(residual, mlp_gain)
        residual = residual + expert_mix(normed, expert_ids, expert_gates, gate_weight, up_weight, down_weight)
        return residual, None

    final, _ = lax.scan(one_layer, hidden_in.astype(jnp.float32), (w_query, w_key, w_value, w_out, w_gate, w_up, w_down, gain_attn, gain_mlp))
    return final
```

```python
import functools

import jax
import jax.numpy as jnp
from jax import lax
from jax.experimental import pallas as pl
from jax.experimental.pallas import tpu as pltpu
from jax.sharding import PartitionSpec as P

EPS = 1e-5
ROPE_BASE = 10000.0
BLOCK = 256
TILE = 256
BATCH = 16
MASKED = -1e30


def rms_norm(residual, gain):
    inv_rms = lax.rsqrt(jnp.mean(residual * residual, axis=-1, keepdims=True) + EPS)
    return (residual * inv_rms * gain.astype(jnp.float32)).astype(jnp.bfloat16)


def request_starts(seg_rows):
    token_index = jnp.arange(seg_rows.shape[0], dtype=jnp.int32)
    is_start = jnp.concatenate([jnp.ones((1,), dtype=jnp.bool_), seg_rows[1:] != seg_rows[:-1]])
    return lax.cummax(jnp.where(is_start, token_index, 0), axis=0)


def rope_tables(positions, head_dim):
    half = head_dim // 2
    lane = jnp.arange(2 * head_dim, dtype=jnp.int32)
    inv_freq = jnp.power(ROPE_BASE, -(lane % half).astype(jnp.float32) * 2.0 / head_dim)
    angles = positions.astype(jnp.float32)[:, None] * inv_freq[None, :]
    sign = jnp.where(lane % head_dim < half, -1.0, 1.0).astype(jnp.float32)
    return jnp.cos(angles), jnp.sin(angles) * sign


def attention_kernel(lo_ref, mid_ref, h_ref, cos_ref, sin_ref, pos_ref, w_ref, out_ref,
                     k_scr, v_scr, q_scr, m_scr, l_scr, acc_scr, *, pairs, head_dim):
    i = pl.program_id(0)
    width = 2 * head_dim
    span = pairs * width
    half = head_dim // 2
    lane = lax.broadcasted_iota(jnp.int32, (BLOCK, width), 1)
    low_half = lane % head_dim < half
    first_head = lane < head_dim
    cosines = cos_ref[...]
    sines = sin_ref[...]
    h_block = h_ref[...]
    row0 = pl.multiple_of(i * BLOCK, BLOCK)
    for p in range(pairs):
        cols = pl.ds(p * width, width)
        q = jnp.dot(h_block, w_ref[:, pl.ds(p * width, width)], preferred_element_type=jnp.float32)
        k = jnp.dot(h_block, w_ref[:, pl.ds(span + p * width, width)], preferred_element_type=jnp.float32)
        v = jnp.dot(h_block, w_ref[:, pl.ds(2 * span + p * width, width)], preferred_element_type=jnp.float32)
        q_turn = jnp.where(low_half, pltpu.roll(q, width - half, 1), pltpu.roll(q, half, 1))
        k_turn = jnp.where(low_half, pltpu.roll(k, width - half, 1), pltpu.roll(k, half, 1))
        q_rot = (q * cosines + q_turn * sines).astype(jnp.bfloat16).astype(jnp.float32) * (head_dim ** -0.5)
        k_rot = (k * cosines + k_turn * sines).astype(jnp.bfloat16)
        q_scr[2 * p] = jnp.where(first_head, q_rot, 0.0).astype(jnp.bfloat16)
        q_scr[2 * p + 1] = jnp.where(first_head, 0.0, q_rot).astype(jnp.bfloat16)
        k_scr[p, pl.ds(row0, BLOCK), :] = k_rot
        v_scr[p, pl.ds(2 * row0, BLOCK), :] = jnp.where(first_head, v, 0.0).astype(jnp.bfloat16)
        v_scr[p, pl.ds(2 * row0 + BLOCK, BLOCK), :] = jnp.where(first_head, 0.0, v).astype(jnp.bfloat16)

    m_scr[...] = jnp.full_like(m_scr, MASKED)
    l_scr[...] = jnp.zeros_like(l_scr)
    acc_scr[...] = jnp.zeros_like(acc_scr)

    def step(j, masked):
        col0 = pl.multiple_of(j * BLOCK, BLOCK)
        if masked:
            gap = (lax.broadcasted_iota(jnp.int32, (BLOCK, BLOCK), 0) - lax.broadcasted_iota(jnp.int32, (BLOCK, BLOCK), 1)) + (row0 - col0)
            allowed = (gap >= 0) & (gap <= pos_ref[...])
        for p in range(pairs):
            k_block = k_scr[p, pl.ds(col0, BLOCK), :]
            probs = []
            scales = []
            for e in range(2):
                hd = 2 * p + e
                s = lax.dot_general(q_scr[hd], k_block, (((1,), (1,)), ((), ())), preferred_element_type=jnp.float32)
                if masked:
                    s = jnp.where(allowed, s, MASKED)
                m_old = m_scr[hd]
                m_new = jnp.maximum(m_old, jnp.max(s, axis=1, keepdims=True))
                alpha = jnp.exp(m_old - m_new)
                m_wide = jnp.concatenate([m_new] * (BLOCK // width), axis=1)
                e_s = jnp.exp(s - m_wide)
                if masked:
                    e_s = jnp.where(allowed, e_s, 0.0)
                part = e_s[:, :width]
                for c in range(1, BLOCK // width):
                    part = part + e_s[:, c * width:(c + 1) * width]
                l_scr[hd] = l_scr[hd] * alpha + part
                m_scr[hd] = m_new
                probs.append(e_s.astype(jnp.bfloat16))
                scales.append(alpha)
            pv = jnp.dot(jnp.concatenate(probs, axis=1), v_scr[p, pl.ds(2 * col0, 2 * BLOCK), :], preferred_element_type=jnp.float32)
            acc_scr[p] = acc_scr[p] * jnp.where(first_head, scales[0], scales[1]) + pv

    def masked_step(j, carry):
        step(j, True)
        return carry

    def plain_step(j, carry):
        step(j, False)
        return carry

    lax.fori_loop(lo_ref[i], mid_ref[i], masked_step, 0)
    lax.fori_loop(mid_ref[i], i, plain_step, 0)
    step(i, True)

    outs = []
    for p in range(pairs):
        l0 = jnp.sum(l_scr[2 * p], axis=1, keepdims=True)
        l1 = jnp.sum(l_scr[2 * p + 1], axis=1, keepdims=True)
        outs.append((acc_scr[p] / jnp.where(first_head, l0, l1)).astype(jnp.bfloat16))
    o = jnp.concatenate(outs, axis=1)
    out_ref[...] = lax.dot_general(o, w_ref[:, pl.ds(3 * span, span)], (((1,), (1,)), ((), ())), preferred_element_type=jnp.float32)


def attention(normed, weight, cosines, sines, positions, lo, mid, heads, head_dim):
    seq, hidden = normed.shape
    pairs = heads // 2
    width = 2 * head_dim
    blocks = seq // BLOCK
    span = pairs * width
    flops = 2 * seq * hidden * 4 * span + 4 * seq * (seq // 4) * span
    return pl.pallas_call(
        functools.partial(attention_kernel, pairs=pairs, head_dim=head_dim),
        name='attn',
        out_shape=jax.ShapeDtypeStruct((seq, hidden), jnp.float32),
        grid_spec=pltpu.PrefetchScalarGridSpec(
            num_scalar_prefetch=2,
            grid=(blocks,),
            in_specs=[
                pl.BlockSpec((BLOCK, hidden), lambda i, *_: (i, 0)),
                pl.BlockSpec((BLOCK, width), lambda i, *_: (i, 0)),
                pl.BlockSpec((BLOCK, width), lambda i, *_: (i, 0)),
                pl.BlockSpec((BLOCK, 1), lambda i, *_: (i, 0)),
                pl.BlockSpec(weight.shape, lambda i, *_: (0, 0)),
            ],
            out_specs=pl.BlockSpec((BLOCK, hidden), lambda i, *_: (i, 0)),
            scratch_shapes=[
                pltpu.VMEM((pairs, seq, width), jnp.bfloat16),
                pltpu.VMEM((pairs, 2 * seq, width), jnp.bfloat16),
                pltpu.VMEM((heads, BLOCK, width), jnp.bfloat16),
                pltpu.VMEM((heads, BLOCK, width), jnp.float32),
                pltpu.VMEM((heads, BLOCK, width), jnp.float32),
                pltpu.VMEM((pairs, BLOCK, width), jnp.float32),
            ],
        ),
        compiler_params=pltpu.CompilerParams(dimension_semantics=('arbitrary',), vmem_limit_bytes=48 * 1024 * 1024),
        cost_estimate=pl.CostEstimate(flops=flops, bytes_accessed=6 * seq * hidden, transcendentals=seq * (seq // 4) * heads),
    )(lo, mid, normed, cosines, sines, positions, weight)


def moe_kernel(tile_start_ref, tok_ref, gate_ref, h_hbm, wg_ref, wu_ref, wd_ref, out_hbm,
               h_scr, acc_scr, x_scr, y_scr, a_scr, in_scr, out_scr, in_sem, out_sem, *, seq, hidden):
    e = pl.program_id(0)
    last = pl.num_programs(0) - 1
    groups = hidden // 128
    chunks = seq // TILE

    def fetch(c, slot):
        return pltpu.make_async_copy(h_hbm.at[pl.ds(pl.multiple_of(c * TILE, TILE), TILE), :], in_scr.at[slot], in_sem.at[slot])

    @pl.when(e == 0)
    def _():
        fetch(0, 0).start()

        def load(c, carry):
            slot = lax.rem(c, 2)

            @pl.when(c + 1 < chunks)
            def _():
                fetch(c + 1, 1 - slot).start()

            fetch(c, slot).wait()
            rows = in_scr[slot].astype(jnp.float32)
            for g in range(groups):
                h_scr[pl.ds(pl.multiple_of(c * TILE, TILE), TILE), g, :] = rows[:, g * 128:(g + 1) * 128]
            acc_scr[pl.ds(pl.multiple_of(c * TILE, TILE), TILE)] = jnp.zeros((TILE, 8, 128), jnp.float32)
            return carry

        lax.fori_loop(0, chunks, load, 0)
        h_scr[pl.ds(seq, 8)] = jnp.zeros((8, 8, 128), jnp.float32)

    w_gate = wg_ref[...].reshape(hidden, wg_ref.shape[-1])
    w_up = wu_ref[...].reshape(hidden, wu_ref.shape[-1])
    w_down = wd_ref[...].reshape(hidden, wd_ref.shape[-1])
    ffn = wg_ref.shape[-1]
    step_n = 512

    def tile_body(t, carry):
        base = t * TILE

        def gather(b, carry):
            first = base + b * BATCH
            vals = [h_scr[tok_ref[first + r]] for r in range(BATCH)]
            for r in range(BATCH):
                x_scr[b * BATCH + r] = vals[r]
            return carry

        lax.fori_loop(0, TILE // BATCH, gather, 0)
        x = jnp.concatenate([x_scr[:, g, :] for g in range(groups)], axis=1).astype(jnp.bfloat16)
        for n in range(0, ffn, step_n):
            gate_pre = jnp.dot(x, wg_ref[:, 0, :, pl.ds(n, step_n)].reshape(hidden, step_n), preferred_element_type=jnp.float32)
            up_pre = jnp.dot(x, wu_ref[:, 0, :, pl.ds(n, step_n)].reshape(hidden, step_n), preferred_element_type=jnp.float32)
            a_scr[:, pl.ds(n, step_n)] = (gate_pre * jax.nn.sigmoid(gate_pre) * up_pre).astype(jnp.bfloat16)
        y = lax.dot_general(a_scr[...], wd_ref[:, 0].reshape(hidden, ffn), (((1,), (1,)), ((), ())), preferred_element_type=jnp.float32)
        for g in range(groups):
            y_scr[:, g, :] = y[:, g * 128:(g + 1) * 128]

        def scatter(b, carry):
            first = base + b * BATCH
            toks = [tok_ref[first + r] for r in range(BATCH)]
            vals = [acc_scr[toks[r]] + gate_ref[first + r] * y_scr[b * BATCH + r] for r in range(BATCH)]
            for r in range(BATCH):
                acc_scr[toks[r]] = vals[r]
            return carry

        lax.fori_loop(0, TILE // BATCH, scatter, 0)
        return carry

    lax.fori_loop(tile_start_ref[e], tile_start_ref[e + 1], tile_body, 0)

    def flush(c, slot):
        return pltpu.make_async_copy(out_scr.at[slot], out_hbm.at[pl.ds(pl.multiple_of(c * TILE, TILE), TILE), :], out_sem.at[slot])

    @pl.when(e == last)
    def _():
        def store(c, carry):
            slot = lax.rem(c, 2)

            @pl.when(c >= 2)
            def _():
                flush(c - 2, slot).wait()

            for g in range(groups):
                out_scr[slot, :, pl.ds(g * 128, 128)] = acc_scr[pl.ds(pl.multiple_of(c * TILE, TILE), TILE), g, :]
            flush(c, slot).start()
            return carry

        lax.fori_loop(0, chunks, store, 0)
        flush(chunks - 2, lax.rem(chunks - 2, 2)).wait()
        flush(chunks - 1, lax.rem(chunks - 1, 2)).wait()


def expert_mix(normed, tile_start, pair_token, pair_gate, w_gate, w_up, w_down):
    seq, hidden = normed.shape
    parts, experts, depth, ffn = w_gate.shape
    weight_spec = pl.BlockSpec((parts, 1, depth, ffn), lambda e, *_: (0, e, 0, 0))
    return pl.pallas_call(
        functools.partial(moe_kernel, seq=seq, hidden=hidden),
        name='moe',
        out_shape=jax.ShapeDtypeStruct((seq, hidden), jnp.float32),
        grid_spec=pltpu.PrefetchScalarGridSpec(
            num_scalar_prefetch=3,
            grid=(experts,),
            in_specs=[pl.BlockSpec(memory_space=pl.ANY), weight_spec, weight_spec, weight_spec],
            out_specs=pl.BlockSpec(memory_space=pl.ANY),
            scratch_shapes=[
                pltpu.VMEM((seq + 8, 8, 128), jnp.float32),
                pltpu.VMEM((seq + 8, 8, 128), jnp.float32),
                pltpu.VMEM((TILE, 8, 128), jnp.float32),
                pltpu.VMEM((TILE, 8, 128), jnp.float32),
                pltpu.VMEM((TILE, ffn), jnp.bfloat16),
                pltpu.VMEM((2, TILE, hidden), jnp.bfloat16),
                pltpu.VMEM((2, TILE, hidden), jnp.float32),
                pltpu.SemaphoreType.DMA((2,)),
                pltpu.SemaphoreType.DMA((2,)),
            ],
        ),
        compiler_params=pltpu.CompilerParams(dimension_semantics=('arbitrary',), vmem_limit_bytes=63 * 1024 * 1024),
        cost_estimate=pl.CostEstimate(flops=2 * 3 * 2 * seq * hidden * ffn, bytes_accessed=3 * 2 * experts * hidden * ffn + 6 * seq * hidden, transcendentals=2 * seq * ffn),
    )(tile_start, pair_token, pair_gate, normed, w_gate, w_up, w_down)


def route(ids_full, gates_full, num_experts):
    seq = ids_full.shape[0]
    flat_ids = ids_full.reshape(2 * seq)
    sizes = jnp.sum((flat_ids[None, :] == jnp.arange(num_experts, dtype=jnp.int32)[:, None]).astype(jnp.int32), axis=1)
    tiles = (sizes + TILE - 1) // TILE
    tile_start = jnp.concatenate([jnp.zeros((1,), jnp.int32), jnp.cumsum(tiles).astype(jnp.int32)])
    spare = tiles * TILE - sizes
    filler = jnp.arange(TILE, dtype=jnp.int32)[None, :] < spare[:, None]
    filler_key = jnp.where(filler, jnp.arange(num_experts, dtype=jnp.int32)[:, None], num_experts).reshape(num_experts * TILE)
    keys = jnp.concatenate([flat_ids, filler_key])
    tokens = jnp.concatenate([jnp.arange(2 * seq, dtype=jnp.int32) // 2, jnp.full((num_experts * TILE,), seq, jnp.int32)])
    gates = jnp.concatenate([gates_full.reshape(2 * seq), jnp.zeros((num_experts * TILE,), jnp.float32)])
    _, pair_token, pair_gate = lax.sort((keys, tokens, gates), num_keys=1, is_stable=True)
    return tile_start, pair_token, pair_gate


def solution(mesh):
    token_spec = P(('rep', 'tok', 'mp'))
    row_spec = P(('rep', 'tok', 'mp'), None)
    head_weight = P(None, 'tok', 'mp', None)
    in_specs = (row_spec, token_spec, row_spec, row_spec, head_weight, head_weight, head_weight, P(None, 'mp', None, 'tok'), P(None, None, 'tok', 'mp'), P(None, None, 'tok', 'mp'), P(None, None, 'mp', 'tok'), P(None, None), P(None, None))

    def device_step(hidden_in, seg_ids, expert_ids, expert_gates, w_query, w_key, w_value, w_out, w_gate, w_up, w_down, gain_attn, gain_mlp):
        num_layers, depth, heads, head_dim = w_query.shape
        num_experts = w_gate.shape[1]
        hidden = hidden_in.shape[1]
        own_rows = hidden_in.shape[0]
        swap = [(0, 1), (1, 0)]
        my_mp = lax.axis_index('mp')

        seg_full = lax.all_gather(seg_ids, 'mp', axis=0, tiled=True)
        ids_full = lax.all_gather(expert_ids, 'mp', axis=0, tiled=True)
        gates_full = lax.all_gather(expert_gates, 'mp', axis=0, tiled=True)
        seq_len = seg_full.shape[0]
        starts = request_starts(seg_full)
        positions = jnp.arange(seq_len, dtype=jnp.int32) - starts
        cosines, sines = rope_tables(positions, head_dim)
        blocked = starts.reshape(seq_len // BLOCK, BLOCK)
        lo = blocked[:, 0] // BLOCK
        mid = jnp.minimum((blocked[:, -1] + BLOCK - 1) // BLOCK, jnp.arange(seq_len // BLOCK, dtype=jnp.int32))
        mid = jnp.maximum(mid, lo)
        tile_start, pair_token, pair_gate = route(ids_full, gates_full, num_experts)

        def combine(residual, part):
            own = lax.dynamic_slice(part, (my_mp * own_rows, 0), (own_rows, hidden))
            away = lax.dynamic_slice(part, ((1 - my_mp) * own_rows, 0), (own_rows, hidden)).astype(jnp.bfloat16)
            return residual + (own + lax.ppermute(away, 'mp', swap).astype(jnp.float32))

        residual = hidden_in.astype(jnp.float32)
        for layer in range(num_layers):
            packed = jnp.concatenate([
                w_query[layer].reshape(depth, heads * head_dim),
                w_key[layer].reshape(depth, heads * head_dim),
                w_value[layer].reshape(depth, heads * head_dim),
                w_out[layer].reshape(heads * head_dim, depth).T,
            ], axis=1)
            attn_weight = lax.all_gather(packed, 'tok', axis=0, tiled=True)
            gate_weight = lax.all_gather(w_gate[layer], 'tok', axis=0)
            up_weight = lax.all_gather(w_up[layer], 'tok', axis=0)
            down_weight = lax.all_gather(jnp.swapaxes(w_down[layer], 1, 2), 'tok', axis=0)
            normed = lax.all_gather(rms_norm(residual, gain_attn[layer]), 'mp', axis=0, tiled=True)
            attn_part = attention(normed, attn_weight, cosines, sines, positions[:, None], lo, mid, heads, head_dim)
            residual = combine(residual, attn_part)
            normed = lax.all_gather(rms_norm(residual, gain_mlp[layer]), 'mp', axis=0, tiled=True)
            mix_part = expert_mix(normed, tile_start, pair_token, pair_gate, gate_weight, up_weight, down_weight)
            residual = combine(residual, mix_part)
        return residual

    return jax.shard_map(device_step, mesh=mesh, in_specs=in_specs, out_specs=row_spec, check_vma=False)
```

```python
import functools

import jax
import jax.numpy as jnp
from jax import lax
from jax.experimental import pallas as pl
from jax.experimental.pallas import tpu as pltpu
from jax.sharding import PartitionSpec as P


EPS = 1e-5
ROPE_BASE = 10000.0
BLOCK = 256
TILE = 256
BATCH = 16
MASKED = -1e30


def rms_norm(residual, gain):
    inv_rms = lax.rsqrt(jnp.mean(residual * residual, axis=-1, keepdims=True) + EPS)
    return (residual * inv_rms * gain.astype(jnp.float32)).astype(jnp.bfloat16)


def request_starts(seg_rows):
    token_index = jnp.arange(seg_rows.shape[0], dtype=jnp.int32)
    is_start = jnp.concatenate([jnp.ones((1,), dtype=jnp.bool_), seg_rows[1:] != seg_rows[:-1]])
    return lax.cummax(jnp.where(is_start, token_index, 0), axis=0)


def rope_tables(positions, head_dim):
    half = head_dim // 2
    lane = jnp.arange(2 * head_dim, dtype=jnp.int32)
    inv_freq = jnp.power(ROPE_BASE, -(lane % half).astype(jnp.float32) * 2.0 / head_dim)
    angles = positions.astype(jnp.float32)[:, None] * inv_freq[None, :]
    sign = jnp.where(lane % head_dim < half, -1.0, 1.0).astype(jnp.float32)
    return jnp.cos(angles), jnp.sin(angles) * sign


def attention_kernel(place_ref, lo_ref, mid_ref, own_ref, other_ref, cos_ref, sin_ref, pos_ref, w0, w1, w2, w3,
                     keep_ref, send_ref, w_scr, k_scr, v_scr, q_scr, m_scr, l_scr, acc_scr, w_sem, *, pairs, head_dim):
    i = pl.program_id(0)
    mine = place_ref[1] == i // (pl.num_programs(0) // 2)
    width = 2 * head_dim
    span = pairs * width
    half = head_dim // 2
    hidden = w_scr.shape[0] * w_scr.shape[1]

    @pl.when(i == 0)
    def _():
        copies = [pltpu.make_async_copy(piece, w_scr.at[place_ref[2 + q]], w_sem) for q, piece in enumerate((w0, w1, w2, w3))]
        for copy in copies:
            copy.start()
        for copy in copies:
            copy.wait()

    lane = lax.broadcasted_iota(jnp.int32, (BLOCK, width), 1)
    low_half = lane % head_dim < half
    first_head = lane < head_dim
    cosines = cos_ref[...]
    sines = sin_ref[...]
    h_block = jnp.where(mine, own_ref[...], other_ref[...])
    row0 = pl.multiple_of(i * BLOCK, BLOCK)

    def weight(col):
        return w_scr[:, :, pl.ds(col, width)].reshape(hidden, width)

    for p in range(pairs):
        q = jnp.dot(h_block, weight(p * width), preferred_element_type=jnp.float32)
        k = jnp.dot(h_block, weight(span + p * width), preferred_element_type=jnp.float32)
        v = jnp.dot(h_block, weight(2 * span + p * width), preferred_element_type=jnp.float32)
        q_turn = jnp.where(low_half, pltpu.roll(q, width - half, 1), pltpu.roll(q, half, 1))
        k_turn = jnp.where(low_half, pltpu.roll(k, width - half, 1), pltpu.roll(k, half, 1))
        q_rot = (q * cosines + q_turn * sines).astype(jnp.bfloat16).astype(jnp.float32) * (head_dim ** -0.5)
        k_rot = (k * cosines + k_turn * sines).astype(jnp.bfloat16)
        q_scr[2 * p] = jnp.where(first_head, q_rot, 0.0).astype(jnp.bfloat16)
        q_scr[2 * p + 1] = jnp.where(first_head, 0.0, q_rot).astype(jnp.bfloat16)
        k_scr[p, pl.ds(row0, BLOCK), :] = k_rot
        v_scr[p, pl.ds(2 * row0, BLOCK), :] = jnp.where(first_head, v, 0.0).astype(jnp.bfloat16)
        v_scr[p, pl.ds(2 * row0 + BLOCK, BLOCK), :] = jnp.where(first_head, 0.0, v).astype(jnp.bfloat16)

    m_scr[...] = jnp.full_like(m_scr, MASKED)
    l_scr[...] = jnp.zeros_like(l_scr)
    acc_scr[...] = jnp.zeros_like(acc_scr)

    def step(j, masked):
        col0 = pl.multiple_of(j * BLOCK, BLOCK)
        if masked:
            gap = (lax.broadcasted_iota(jnp.int32, (BLOCK, BLOCK), 0) - lax.broadcasted_iota(jnp.int32, (BLOCK, BLOCK), 1)) + (row0 - col0)
            allowed = (gap >= 0) & (gap <= pos_ref[...])
        for p in range(pairs):
            k_block = k_scr[p, pl.ds(col0, BLOCK), :]
            probs = []
            scales = []
            for e in range(2):
                hd = 2 * p + e
                s = lax.dot_general(q_scr[hd], k_block, (((1,), (1,)), ((), ())), preferred_element_type=jnp.float32)
                if masked:
                    s = jnp.where(allowed, s, MASKED)
                m_old = m_scr[hd]
                m_new = jnp.maximum(m_old, jnp.max(s, axis=1, keepdims=True))
                alpha = jnp.exp(m_old - m_new)
                m_wide = jnp.concatenate([m_new] * (BLOCK // width), axis=1)
                e_s = jnp.exp(s - m_wide)
                if masked:
                    e_s = jnp.where(allowed, e_s, 0.0)
                part = e_s[:, :width]
                for c in range(1, BLOCK // width):
                    part = part + e_s[:, c * width:(c + 1) * width]
                l_scr[hd] = l_scr[hd] * alpha + part
                m_scr[hd] = m_new
                probs.append(e_s.astype(jnp.bfloat16))
                scales.append(alpha)
            pv = jnp.dot(jnp.concatenate(probs, axis=1), v_scr[p, pl.ds(2 * col0, 2 * BLOCK), :], preferred_element_type=jnp.float32)
            acc_scr[p] = acc_scr[p] * jnp.where(first_head, scales[0], scales[1]) + pv

    def masked_step(j, carry):
        step(j, True)
        return carry

    def plain_step(j, carry):
        step(j, False)
        return carry

    lax.fori_loop(lo_ref[i], mid_ref[i], masked_step, 0)
    lax.fori_loop(mid_ref[i], i, plain_step, 0)
    step(i, True)

    outs = []
    for p in range(pairs):
        l0 = jnp.sum(l_scr[2 * p], axis=1, keepdims=True)
        l1 = jnp.sum(l_scr[2 * p + 1], axis=1, keepdims=True)
        outs.append((acc_scr[p] / jnp.where(first_head, l0, l1)).astype(jnp.bfloat16))
    o = jnp.concatenate(outs, axis=1)
    w_o = w_scr[:, :, pl.ds(3 * span, span)].reshape(hidden, span)
    out = lax.dot_general(o, w_o, (((1,), (1,)), ((), ())), preferred_element_type=jnp.float32)

    @pl.when(mine)
    def _():
        keep_ref[...] = out

    @pl.when(jnp.logical_not(mine))
    def _():
        send_ref[...] = out.astype(jnp.bfloat16)


def attention(own, other, pieces, cosines, sines, positions, place, lo, mid, heads, head_dim):
    rows, hidden = own.shape
    seq = 2 * rows
    pairs = heads // 2
    width = 2 * head_dim
    blocks = seq // BLOCK
    span = pairs * width
    per = blocks // 2
    flops = 2 * seq * hidden * 4 * span + 4 * seq * (seq // 4) * span

    def own_index(i, place, *_):
        return (jnp.clip(i - per * place[1], 0, per - 1), 0)

    def other_index(i, place, *_):
        return (jnp.clip(i - per * (1 - place[1]), 0, per - 1), 0)

    anywhere = pl.BlockSpec(memory_space=pl.ANY)
    return pl.pallas_call(
        functools.partial(attention_kernel, pairs=pairs, head_dim=head_dim),
        name='attn',
        out_shape=(jax.ShapeDtypeStruct((rows, hidden), jnp.float32), jax.ShapeDtypeStruct((rows, hidden), jnp.bfloat16)),
        grid_spec=pltpu.PrefetchScalarGridSpec(
            num_scalar_prefetch=3,
            grid=(blocks,),
            in_specs=[
                pl.BlockSpec((BLOCK, hidden), own_index),
                pl.BlockSpec((BLOCK, hidden), other_index),
                pl.BlockSpec((BLOCK, width), lambda i, *_: (i, 0)),
                pl.BlockSpec((BLOCK, width), lambda i, *_: (i, 0)),
                pl.BlockSpec((BLOCK, 1), lambda i, *_: (i, 0)),
                anywhere, anywhere, anywhere, anywhere,
            ],
            out_specs=(pl.BlockSpec((BLOCK, hidden), own_index), pl.BlockSpec((BLOCK, hidden), other_index)),
            scratch_shapes=[
                pltpu.VMEM((len(pieces),) + pieces[0].shape, jnp.bfloat16),
                pltpu.VMEM((pairs, seq, width), jnp.bfloat16),
                pltpu.VMEM((pairs, 2 * seq, width), jnp.bfloat16),
                pltpu.VMEM((heads, BLOCK, width), jnp.bfloat16),
                pltpu.VMEM((heads, BLOCK, width), jnp.float32),
                pltpu.VMEM((heads, BLOCK, width), jnp.float32),
                pltpu.VMEM((pairs, BLOCK, width), jnp.float32),
                pltpu.SemaphoreType.DMA,
            ],
        ),
        compiler_params=pltpu.CompilerParams(dimension_semantics=('arbitrary',), vmem_limit_bytes=48 * 1024 * 1024),
        cost_estimate=pl.CostEstimate(flops=flops, bytes_accessed=6 * seq * hidden, transcendentals=seq * (seq // 4) * heads),
    )(place, lo, mid, own, other, cosines, sines, positions, *pieces)


def moe_kernel(place_ref, tile_start_ref, tok_ref, gate_ref, *refs, seq, hidden, base_expert, experts, first, last):
    own_hbm, other_hbm, w0, w1, w2, w3 = refs[:6]
    refs = refs[6:]
    if not first:
        acc_in, refs = refs[0], refs[1:]
    if last:
        keep_hbm, send_hbm = refs[:2]
        refs = refs[2:]
    else:
        acc_out, refs = refs[0], refs[1:]
    h_scr, acc_scr, x_scr, y_scr, a_scr, w_scr, in_scr, keep_scr, send_scr, in_sem, keep_sem, send_sem, w_sem, acc_sem = refs
    groups = hidden // 128
    chunks = seq // TILE
    half = chunks // 2
    ffn = w_scr.shape[-1]
    step_n = 512
    my_mp = place_ref[1]
    pieces = (w0, w1, w2, w3)

    def rows_of(c):
        return pl.ds(pl.multiple_of(c * TILE, TILE), TILE)

    def weights(e, slot):
        copies = []
        for q, piece in enumerate(pieces):
            for t in range(3):
                copies.append(pltpu.make_async_copy(piece.at[t * experts + e], w_scr.at[slot, t, place_ref[2 + q]], w_sem.at[slot]))
        return copies

    for copy in weights(0, 0):
        copy.start()
    if not first:
        acc_copy = pltpu.make_async_copy(acc_in, acc_scr.at[pl.ds(0, seq)], acc_sem)
        acc_copy.start()

    def fetch(c, slot, act):
        mine = my_mp == c // half
        local = lax.rem(c, half)

        @pl.when(mine)
        def _():
            act(pltpu.make_async_copy(own_hbm.at[rows_of(local), :], in_scr.at[slot], in_sem.at[slot]))

        @pl.when(jnp.logical_not(mine))
        def _():
            act(pltpu.make_async_copy(other_hbm.at[rows_of(local), :], in_scr.at[slot], in_sem.at[slot]))

    fetch(0, 0, lambda copy: copy.start())

    def load(c, carry):
        slot = lax.rem(c, 2)

        @pl.when(c + 1 < chunks)
        def _():
            fetch(c + 1, 1 - slot, lambda copy: copy.start())

        fetch(c, slot, lambda copy: copy.wait())
        rows = in_scr[slot].astype(jnp.float32)
        for g in range(groups):
            h_scr[rows_of(c), g, :] = rows[:, g * 128:(g + 1) * 128]
        if first:
            acc_scr[rows_of(c)] = jnp.zeros((TILE, 8, 128), jnp.float32)
        return carry

    lax.fori_loop(0, chunks, load, 0)
    h_scr[pl.ds(seq, 8)] = jnp.zeros((8, 8, 128), jnp.float32)
    acc_scr[pl.ds(seq, 8)] = jnp.zeros((8, 8, 128), jnp.float32)
    if not first:
        acc_copy.wait()

    def gather(t, slot, lo, hi):
        first_row = t * TILE
        for b in range(lo, hi, BATCH):
            vals = [h_scr[tok_ref[first_row + b + r]] for r in range(BATCH)]
            for r in range(BATCH):
                x_scr[slot, b + r] = vals[r]

    def scatter(t, slot, lo, hi):
        first_row = t * TILE
        for b in range(lo, hi, BATCH):
            toks = [tok_ref[first_row + b + r] for r in range(BATCH)]
            vals = [acc_scr[toks[r]] + gate_ref[first_row + b + r] * y_scr[slot, b + r] for r in range(BATCH)]
            for r in range(BATCH):
                acc_scr[toks[r]] = vals[r]

    begin = tile_start_ref[base_expert]
    end = tile_start_ref[base_expert + experts]
    y_scr[lax.rem(begin + 1, 2)] = jnp.zeros(y_scr.shape[1:], jnp.float32)

    def gather_loop(b, carry):
        vals = [h_scr[tok_ref[begin * TILE + b * BATCH + r]] for r in range(BATCH)]
        for r in range(BATCH):
            x_scr[lax.rem(begin, 2), b * BATCH + r] = vals[r]
        return carry

    lax.fori_loop(0, TILE // BATCH, gather_loop, 0)

    def expert_body(e, carry):
        slot_w = lax.rem(e, 2)

        @pl.when(e + 1 < experts)
        def _():
            for copy in weights(e + 1, 1 - slot_w):
                copy.start()

        for copy in weights(e, slot_w):
            copy.wait()

        def tile_body(t, carry):
            slot = lax.rem(t, 2)
            before = jnp.maximum(t - 1, 0)
            x = jnp.concatenate([x_scr[slot, :, g, :] for g in range(groups)], axis=1).astype(jnp.bfloat16)
            parts = ffn // step_n
            cut = [TILE * n // parts // BATCH * BATCH for n in range(parts)] + [TILE]
            for n in range(parts):
                cols = pl.ds(n * step_n, step_n)
                gate_pre = jnp.dot(x, w_scr[slot_w, 0, :, :, cols].reshape(hidden, step_n), preferred_element_type=jnp.float32)
                up_pre = jnp.dot(x, w_scr[slot_w, 1, :, :, cols].reshape(hidden, step_n), preferred_element_type=jnp.float32)
                a_scr[:, cols] = (gate_pre * jax.nn.sigmoid(gate_pre) * up_pre).astype(jnp.bfloat16)
                scatter(before, 1 - slot, cut[n], cut[n + 1])
                gather(t + 1, 1 - slot, cut[n], cut[n + 1])
            y = lax.dot_general(a_scr[...], w_scr[slot_w, 2].reshape(hidden, ffn), (((1,), (1,)), ((), ())), preferred_element_type=jnp.float32)
            for g in range(groups):
                y_scr[slot, :, g, :] = y[:, g * 128:(g + 1) * 128]
            return carry

        lax.fori_loop(tile_start_ref[base_expert + e], tile_start_ref[base_expert + e + 1], tile_body, 0)
        return carry

    lax.fori_loop(0, experts, expert_body, 0)

    @pl.when(end > begin)
    def _():
        final = end - 1

        def scatter_loop(b, carry):
            first_row = final * TILE + b * BATCH
            toks = [tok_ref[first_row + r] for r in range(BATCH)]
            vals = [acc_scr[toks[r]] + gate_ref[first_row + r] * y_scr[lax.rem(final, 2), b * BATCH + r] for r in range(BATCH)]
            for r in range(BATCH):
                acc_scr[toks[r]] = vals[r]
            return carry

        lax.fori_loop(0, TILE // BATCH, scatter_loop, 0)

    if not last:
        copy = pltpu.make_async_copy(acc_scr.at[pl.ds(0, seq)], acc_out, acc_sem)
        copy.start()
        copy.wait()
        return

    def flush(scr, hbm, sem, c, slot):
        return pltpu.make_async_copy(scr.at[slot], hbm.at[rows_of(c), :], sem.at[slot])

    for which, (scr, hbm, sem) in enumerate(((send_scr, send_hbm, send_sem), (keep_scr, keep_hbm, keep_sem))):
        offset = (my_mp if which else 1 - my_mp) * half

        def store(c, carry, scr=scr, hbm=hbm, sem=sem, offset=offset):
            slot = lax.rem(c, 2)

            @pl.when(c >= 2)
            def _():
                flush(scr, hbm, sem, c - 2, slot).wait()

            for g in range(groups):
                scr[slot, :, pl.ds(g * 128, 128)] = acc_scr[rows_of(offset + c), g, :].astype(scr.dtype)
            flush(scr, hbm, sem, c, slot).start()
            return carry

        lax.fori_loop(0, half, store, 0)
        for c in (half - 2, half - 1):
            flush(scr, hbm, sem, c, c % 2).wait()


def expert_mix(own, other, place, tile_start, pair_token, pair_gate, pieces, base_expert, acc, last):
    rows, hidden = own.shape
    seq = 2 * rows
    experts = pieces[0].shape[0] // 3
    depth, ffn = pieces[0].shape[1:]
    anywhere = pl.BlockSpec(memory_space=pl.ANY)
    first = acc is None
    operands = [own, other, *pieces] + ([] if first else [acc])
    if last:
        out_shape = (jax.ShapeDtypeStruct((rows, hidden), jnp.float32), jax.ShapeDtypeStruct((rows, hidden), jnp.bfloat16))
        out_specs = (anywhere, anywhere)
    else:
        out_shape = jax.ShapeDtypeStruct((seq, 8, 128), jnp.float32)
        out_specs = anywhere
    return pl.pallas_call(
        functools.partial(moe_kernel, seq=seq, hidden=hidden, base_expert=base_expert, experts=experts, first=first, last=last),
        name='moe',
        out_shape=out_shape,
        grid_spec=pltpu.PrefetchScalarGridSpec(
            num_scalar_prefetch=4,
            grid=(1,),
            in_specs=[anywhere] * len(operands),
            out_specs=out_specs,
            scratch_shapes=[
                pltpu.VMEM((seq + 8, 8, 128), jnp.float32),
                pltpu.VMEM((seq + 8, 8, 128), jnp.float32),
                pltpu.VMEM((2, TILE, 8, 128), jnp.float32),
                pltpu.VMEM((2, TILE, 8, 128), jnp.float32),
                pltpu.VMEM((TILE, ffn), jnp.bfloat16),
                pltpu.VMEM((2, 3, len(pieces), depth, ffn), jnp.bfloat16),
                pltpu.VMEM((2, TILE, hidden), jnp.bfloat16),
                pltpu.VMEM((2, TILE, hidden), jnp.float32),
                pltpu.VMEM((2, TILE, hidden), jnp.bfloat16),
                pltpu.SemaphoreType.DMA((2,)),
                pltpu.SemaphoreType.DMA((2,)),
                pltpu.SemaphoreType.DMA((2,)),
                pltpu.SemaphoreType.DMA((2,)),
                pltpu.SemaphoreType.DMA,
            ],
        ),
        compiler_params=pltpu.CompilerParams(dimension_semantics=('arbitrary',), vmem_limit_bytes=63 * 1024 * 1024),
        cost_estimate=pl.CostEstimate(flops=3 * 2 * seq * hidden * ffn, bytes_accessed=6 * experts * hidden * ffn + 20 * seq * hidden, transcendentals=seq * ffn),
    )(place, tile_start, pair_token, pair_gate, *operands)


def route(ids_full, gates_full, num_experts):
    seq = ids_full.shape[0]
    flat_ids = ids_full.reshape(2 * seq)
    sizes = jnp.sum((flat_ids[None, :] == jnp.arange(num_experts, dtype=jnp.int32)[:, None]).astype(jnp.int32), axis=1)
    tiles = (sizes + TILE - 1) // TILE
    tile_start = jnp.concatenate([jnp.zeros((1,), jnp.int32), jnp.cumsum(tiles).astype(jnp.int32)])
    spare = tiles * TILE - sizes
    filler = jnp.arange(TILE, dtype=jnp.int32)[None, :] < spare[:, None]
    filler_key = jnp.where(filler, jnp.arange(num_experts, dtype=jnp.int32)[:, None], num_experts).reshape(num_experts * TILE)
    keys = jnp.concatenate([flat_ids, filler_key])
    tokens = jnp.concatenate([jnp.arange(2 * seq, dtype=jnp.int32) // 2, jnp.full((num_experts * TILE,), seq, jnp.int32)])
    gates = jnp.concatenate([gates_full.reshape(2 * seq), jnp.zeros((num_experts * TILE,), jnp.float32)])
    _, pair_token, pair_gate = lax.sort((keys, tokens, gates), num_keys=1, is_stable=True)
    return tile_start, pair_token, pair_gate


def solution(mesh):
    token_spec = P(('rep', 'tok', 'mp'))
    row_spec = P(('rep', 'tok', 'mp'), None)
    head_weight = P(None, 'tok', 'mp', None)
    in_specs = (row_spec, token_spec, row_spec, row_spec, head_weight, head_weight, head_weight, P(None, 'mp', None, 'tok'), P(None, None, 'tok', 'mp'), P(None, None, 'tok', 'mp'), P(None, None, 'mp', 'tok'), P(None, None), P(None, None))

    def device_step(hidden_in, seg_ids, expert_ids, expert_gates, w_query, w_key, w_value, w_out, w_gate, w_up, w_down, gain_attn, gain_mlp):
        num_layers, depth, heads, head_dim = w_query.shape
        num_experts = w_gate.shape[1]
        halves = 2
        group = num_experts // halves
        swap = [(0, 1), (1, 0)]
        across = [(t, t ^ 2) for t in range(4)]
        beside = [(t, t ^ 1) for t in range(4)]
        my_mp = lax.axis_index('mp')
        my_tok = lax.axis_index('tok')
        place = jnp.stack([my_tok, my_mp] + [my_tok ^ q for q in range(4)]).astype(jnp.int32)

        def spread(own):
            far = lax.ppermute(own, 'tok', across)
            side = lax.ppermute(own, 'tok', beside)
            near = lax.ppermute(far, 'tok', beside)
            return own, side, far, near

        def exchange(rows):
            return lax.ppermute(rows, 'mp', swap)

        def pack_attn(layer):
            return jnp.concatenate([
                w_query[layer].reshape(depth, heads * head_dim),
                w_key[layer].reshape(depth, heads * head_dim),
                w_value[layer].reshape(depth, heads * head_dim),
                w_out[layer].reshape(heads * head_dim, depth).T,
            ], axis=1)

        def pack_experts(layer, part):
            which = slice(part * group, (part + 1) * group)
            return jnp.concatenate([w_gate[layer, which], w_up[layer, which], jnp.swapaxes(w_down[layer, which], 1, 2)], axis=0)

        residual = hidden_in.astype(jnp.float32)
        seg_full = lax.all_gather(seg_ids, 'mp', axis=0, tiled=True)
        ids_full = lax.all_gather(expert_ids, 'mp', axis=0, tiled=True)
        gates_full = lax.all_gather(expert_gates, 'mp', axis=0, tiled=True)
        seq_len = seg_full.shape[0]
        starts = request_starts(seg_full)
        positions = jnp.arange(seq_len, dtype=jnp.int32) - starts
        cosines, sines = rope_tables(positions, head_dim)
        blocked = starts.reshape(seq_len // BLOCK, BLOCK)
        lo = blocked[:, 0] // BLOCK
        mid = jnp.minimum((blocked[:, -1] + BLOCK - 1) // BLOCK, jnp.arange(seq_len // BLOCK, dtype=jnp.int32))
        mid = jnp.maximum(mid, lo)
        tile_start, pair_token, pair_gate = route(ids_full, gates_full, num_experts)

        attn_pieces = []
        expert_pieces = []
        for layer in range(num_layers):
            attn_pieces.append(spread(pack_attn(layer)))
            expert_pieces.append([spread(pack_experts(layer, part)) for part in range(halves)])

        for layer in range(num_layers):
            normed = rms_norm(residual, gain_attn[layer])
            other = exchange(normed)
            keep, send = attention(normed, other, attn_pieces[layer], cosines, sines, positions[:, None], place, lo, mid, heads, head_dim)
            residual = residual + (keep + exchange(send).astype(jnp.float32))
            normed = rms_norm(residual, gain_mlp[layer])
            other = exchange(normed)
            acc = None
            for part in range(halves):
                acc = expert_mix(normed, other, place, tile_start, pair_token, pair_gate, expert_pieces[layer][part], part * group, acc, part == halves - 1)
            keep, send = acc
            residual = residual + (keep + exchange(send).astype(jnp.float32))
        return residual


    return jax.shard_map(device_step, mesh=mesh, in_specs=in_specs, out_specs=row_spec, check_vma=False)
```
